1024 devices in a mesh: dp: 8 (over x, core), expert: 128 (over z, y).
Axes of the slice: x: 4, y: 4, z: 32, core: 2. Of those that a mesh axis runs over, the one named last changes fastest.
Arguments:
- tokens: bfloat16 [512, 7168], P('dp', 'expert'), parts along dimension 0, may hold values from -6 to 6
- routes: int32 [512, 8], P('dp'), parts along dimension 0, may hold values from 0 to 15, all different within a row; in each aligned block of 64 rows (0 to 63, 64 to 127, ...) at most 40 rows name the same one
- gate_values: bfloat16 [512, 8], P('dp'), parts along dimension 0, may hold values from 0.049804688 to 1
- gate_weight: bfloat16 [7168, 16384], P(None, 'expert'), may hold values from -0.0625 to 0.0625
- up_weight: bfloat16 [7168, 16384], P(None, 'expert'), may hold values from -0.0625 to 0.0625
- down_weight: bfloat16 [16384, 7168], P(None, 'expert'), may hold values from -0.1875 to 0.1875
Outputs:
- layer_output: bfloat16 [512, 7168], P('dp', 'expert'), parts along dimension 0
The draws below stay inside these ranges and needn't reach their ends.
There are 8 independent parts, one for each index of `dp`. The reference program is written for one: setup_inputs(seed, part) draws one part's arguments, and reference() takes and returns one part's arrays. A program takes and returns all parts, laid end to end along the dimension named above; an argument that names none is the same for every part. Nothing has to cross between parts.
Inputs may be any that keep to these rules, and one draw needn't show every extreme that they name: `routes`: each row names 8 different experts; no expert is named by more than 40 rows of a group, a bound that some block reaches.
All inputs are finite; a program needn't handle non-finite values.
Results may differ from the reference program's by a relative error of at most 0.0049.
Values may be sent and summed in bfloat16 or wider, within the bound.
No kernel may reach another device: no remote copies, remote signals or barrier semaphores. Data moves between devices by JAX's collectives and lax.ppermute only.
A program may use at most 32 MiB of HBM per device.

```python
import math
import jax
import jax.numpy as jnp
import numpy as np
from jax import lax

D = 7168
HIDDEN_SIZE = 1024
EXPERTS = 16
TOPK = 8
TOKENS = 64
CAP = 40


def shard_levels(stream_key, dims, pieces, least, largest):
    loudness = 1.0
    for dim, blocks in pieces:
        heights = jax.random.uniform(jax.random.fold_in(jax.random.fold_in(stream_key, 6), dim), (blocks,), jnp.float32, least / len(pieces), largest / len(pieces))
        loudness = loudness * jnp.repeat(jnp.exp(heights), dims[dim] // blocks).reshape((-1,) + (1,) * (len(dims) - 1 - dim))
    return loudness


def deal_out(own_key, own, number, rows, count, top, bound, skew):
    sequence = jax.random.permutation(own_key, count)
    heavy_load, usual = shares(count, rows * top, bound, skew, True), shares(count, rows * top, bound, skew, False)
    places = jnp.arange(count)

    def named(tallies, offset_by):
        used = int((tallies > 0).sum())
        fixed = max(1, used // 4)
        moved = fixed + (places - fixed + offset_by * (used - fixed)) % max(1, count - fixed)
        return jnp.zeros((count,), jnp.int32).at[sequence[jnp.where(places < fixed, places, moved)]].set(jnp.asarray(tallies, jnp.int32))

    tallies = jnp.where(number % 4 == 0, named(heavy_load, number // 4), named(usual, number - number // 4 - 1))
    mixed = jax.random.permutation(jax.random.fold_in(own, 3), count)
    source_of, sink = mixed[0:count // 2 * 2:2], mixed[1:count // 2 * 2:2]
    slack = jnp.minimum(tallies[source_of] - 1, bound - tallies[sink]) // 2
    slack = jnp.where((source_of == sequence[0]) | (sink == sequence[0]) | (tallies[sink] == 0), 0, jnp.maximum(slack, 0))
    moved = jax.random.randint(jax.random.fold_in(own, 4), (count // 2,), 0, 1 << 20) % (slack + 1)
    tallies = tallies.at[source_of].add(-moved).at[sink].add(moved)
    members = jnp.searchsorted(jnp.cumsum(tallies), jnp.arange(rows * top), side="right").astype(jnp.int32)
    table = members.reshape(top, rows).T
    table = table[jax.random.permutation(jax.random.fold_in(own, 1), rows)]
    offset_by = jax.random.randint(jax.random.fold_in(own, 2), (rows, 1), 0, top)
    return jnp.take_along_axis(table, (jnp.arange(top)[None, :] + offset_by) % top, axis=1)


def shares(count, total, most, lean, full):
    portions = [(1 << 20) // math.isqrt(rank ** lean) + 1 for rank in range(1, count + 1)]
    largest = most if full else min(most, max(-(-total // count), total * portions[0] // sum(portions)))
    least = 1 if total - largest >= count - 1 else 0
    given, surplus = [largest] + [least] * (count - 1), total - largest - least * (count - 1)
    while surplus > 0:
        movable = [i for i in range(1, count) if given[i] < largest] or [i for i in range(1, count) if given[i] < most]
        pool, budget = sum([portions[i] for i in movable]), surplus
        for i in movable:
            extra = min(most - given[i], max(1, budget * portions[i] // pool), surplus)
            given[i] = given[i] + extra
            surplus = surplus - extra
    return np.array(given)


def noise(own_key, dims, spread, most, split=(), kind=jnp.bfloat16):
    entries = spread * jax.random.normal(own_key, dims, jnp.float32)
    if split:
        entries = entries * shard_levels(own_key, dims, split, -0.22, 0.18)
    return jnp.clip(entries, -most, most).astype(kind)


def setup_inputs(seed: int = 0, part: int = 0) -> dict:
    splits = jax.random.split(jax.random.key(seed), 7)
    own_keys = jax.random.split(jax.random.fold_in(splits[6], part), 7)
    tokens = noise(own_keys[0], (TOKENS, D), 1.0, 6.0, ((1, 128),))
    routes_keys = jax.random.split(jax.random.fold_in(own_keys[1], 1), TOKENS // TOKENS)
    routes_turns = jax.random.permutation(jax.random.fold_in(own_keys[1], 3), TOKENS // TOKENS)
    routes = jax.vmap(lambda own, number: deal_out(jax.random.fold_in(own_keys[1], 2), own, number, TOKENS, EXPERTS, TOPK, CAP, 1))(routes_keys, routes_turns).reshape((TOKENS, TOPK))
    gate_values = jnp.clip(jnp.exp(jax.random.uniform(own_keys[2], (TOKENS, TOPK), jnp.float32, math.log(0.049804688), math.log(1.0))), 0.049804688, 1.0).astype(jnp.bfloat16)
    gate_weight = noise(splits[3], (D, EXPERTS * HIDDEN_SIZE), D ** -0.5, 0.0625, ((1, 128),))
    up_weight = noise(splits[4], (D, EXPERTS * HIDDEN_SIZE), D ** -0.5, 0.0625, ((1, 128),))
    down_weight = noise(splits[5], (EXPERTS * HIDDEN_SIZE, D), HIDDEN_SIZE ** -0.5, 0.1875, ((1, 128),))
    return {"tokens": tokens, "routes": routes, "gate_values": gate_values, "gate_weight": gate_weight, "up_weight": up_weight, "down_weight": down_weight}


def reference(tokens, routes, gate_values, gate_weight, up_weight, down_weight):
    expert_ids = jnp.arange(EXPERTS, dtype=jnp.int32)
    matched = routes[:, :, None] == expert_ids[None, None, :]
    combine_table = jnp.sum(jnp.where(matched, gate_values[:, :, None].astype(jnp.float32), jnp.float32(0.0)), axis=1)

    def accumulate(totals, expert):
        first_unit = (expert * HIDDEN_SIZE).astype(jnp.int32)
        gate_slab = lax.dynamic_slice_in_dim(gate_weight, first_unit, HIDDEN_SIZE, 1)
        up_slab = lax.dynamic_slice_in_dim(up_weight, first_unit, HIDDEN_SIZE, 1)
        down_slab = lax.dynamic_slice_in_dim(down_weight, first_unit, HIDDEN_SIZE, 0)
        gate_proj = jnp.dot(tokens, gate_slab, preferred_element_type=jnp.float32)
        up_proj = jnp.dot(tokens, up_slab, preferred_element_type=jnp.float32)
        weight = lax.dynamic_slice_in_dim(combine_table, expert, 1, 1)
        hidden = (jax.nn.silu(gate_proj) * up_proj * weight).astype(jnp.bfloat16)
        return totals + jnp.dot(hidden, down_slab, preferred_element_type=jnp.float32), None

    initial = jnp.zeros((tokens.shape[0], tokens.shape[1]), jnp.float32)
    totals, unused = lax.scan(accumulate, initial, expert_ids)
    return totals.astype(jnp.bfloat16)
```

```python
import jax
import jax.numpy as jnp
from jax import lax
from jax.sharding import Mesh
from jax.sharding import PartitionSpec as P

HIDDEN_SIZE = 1024
EXPERTS = 16
GROUP = ("expert_0", "expert_1", "expert_2")
NEAR = ("expert_1", "expert_2")


def spread(x):
    far = lax.all_gather(x[None], "expert_0", tiled=True)
    near = jnp.broadcast_to(far[None], (8, *far.shape))
    return lax.all_to_all(near, NEAR, 0, 0)


def body(tokens, routes, gate_values, gate_weight, up_weight, down_weight):
    token_count = tokens.shape[0]
    expert = lax.axis_index("expert_0")
    matched = routes[:, :, None] == lax.broadcasted_iota(jnp.int32, (1, 1, EXPERTS), 2)
    combine_table = jnp.sum(
        jnp.where(matched, gate_values[:, :, None].astype(jnp.float32), 0.0), axis=1
    )
    weights = lax.dynamic_slice_in_dim(combine_table, expert, 1, 1)
    capacity = token_count * routes.shape[1] * 5 // (EXPERTS * 4)
    present = combine_table > 0.0
    slot = jnp.cumsum(present.astype(jnp.int32), axis=0) - 1
    placement = jnp.logical_and(
        present[:, :, None],
        slot[:, :, None] == lax.broadcasted_iota(jnp.int32, (1, 1, capacity), 2),
    ).astype(jnp.bfloat16)
    place = lax.dynamic_slice_in_dim(placement, expert, 1, 1)[:, 0, :]

    columns = tokens.T
    packed = jnp.concatenate([columns[:32], jnp.pad(columns[32:], ((0, 8), (0, 0)))], axis=1)
    parts = spread(packed).transpose(1, 0, 2, 3)
    features = jnp.concatenate([parts[..., :64], parts[:, :, :24, 64:]], axis=2)
    features = features.reshape(-1, token_count)
    dims = (((0,), (0,)), ((), ()))
    gate_proj = lax.dot_general(features, gate_weight, dims, preferred_element_type=jnp.float32)
    up_proj = lax.dot_general(features, up_weight, dims, preferred_element_type=jnp.float32)
    hidden = (jax.nn.silu(gate_proj) * up_proj * weights).astype(jnp.bfloat16)
    pieces = lax.dot_general(place, hidden, dims, preferred_element_type=jnp.float32)
    gathered = spread(pieces.astype(jnp.bfloat16))
    full = lax.dot_general(
        placement, gathered, (((2,), (2,)), ((1,), (1,))), preferred_element_type=jnp.float32
    ).astype(jnp.bfloat16)
    full = full.transpose(1, 0, 2, 3).reshape(token_count, -1)
    result = jnp.dot(full, down_weight, preferred_element_type=jnp.float32)
    return result.astype(jnp.bfloat16)


def solution(mesh):
    split = Mesh(
        mesh.devices.reshape(mesh.shape["dp"], 16, 2, 4),
        ("dp", *GROUP),
    )
    return jax.shard_map(
        body,
        mesh=split,
        in_specs=(
            P("dp", GROUP),
            P("dp", None),
            P("dp", None),
            P(None, GROUP),
            P(None, GROUP),
            P(None, GROUP),
        ),
        out_specs=P("dp", GROUP),
        check_vma=False,
    )
```

```python
import jax
import jax.numpy as jnp
from jax import lax
from jax.experimental import pallas as pl
from jax.experimental.pallas import tpu as pltpu
from jax.sharding import Mesh
from jax.sharding import PartitionSpec as P

HIDDEN_SIZE = 1024
EXPERTS = 16
SLOTS = 40
NEAR_SIZE = 8
GROUP = ("expert_0", "expert_1", "expert_2")
NEAR = ("expert_1", "expert_2")
LIMIT = pltpu.CompilerParams(vmem_limit_bytes=32 * 2**20)
F32 = jnp.float32
BF16 = jnp.bfloat16


def dot(x, y, x_dim, y_dim):
    return lax.dot_general(x, y, (((x_dim,), (y_dim,)), ((), ())), preferred_element_type=F32)


def pack_kernel(columns, packed):
    packed[:, :64] = columns[:32]
    packed[:24, 64:] = columns[32:]
    packed[24:, 64:] = jnp.zeros((8, 64), BF16)


def gates_kernel(parts, gate, up, weights, place, pieces):
    low = jnp.zeros((128, 256), F32)
    high = jnp.zeros((128, 256), F32)
    for near in range(NEAR_SIZE):
        x = parts[near].reshape(512, 128)
        w = [ref[:, near, :32, :].reshape(512, 128) for ref in (gate, up)]
        low = low + dot(x, jnp.concatenate(w, axis=1), 0, 0)
        x = parts[near, :, :24, :].reshape(384, 128)
        w = [ref[:, near, 32:, :].reshape(384, 128) for ref in (gate, up)]
        high = high + dot(x, jnp.concatenate(w, axis=1), 0, 0)
    both = low[:64] + high[64:]
    gate_proj, up_proj = both[:, :128], both[:, 128:]
    silu = gate_proj / (1.0 + jnp.exp(-gate_proj))
    hidden = (silu * up_proj * weights[...]).astype(BF16)
    pieces[...] = dot(place[...], hidden, 1, 0).astype(BF16)


def down_kernel(gathered, down, place, out):
    total = jnp.zeros((56, 64), F32)
    for expert in range(EXPERTS):
        for near in range(0, NEAR_SIZE, 2):
            pair = [gathered[near, expert], gathered[near + 1, expert]]
            hidden = dot(place[expert], jnp.concatenate(pair, axis=1), 0, 0).astype(BF16)
            low = expert * HIDDEN_SIZE + near * 128
            total = total + dot(down[:, low : low + 256], hidden, 1, 1)
    out[...] = total.astype(BF16)


def call(kernel, shape, name, *args):
    out = jax.ShapeDtypeStruct(shape, BF16)
    return pl.pallas_call(kernel, out_shape=out, compiler_params=LIMIT, name=name)(*args)


def spread(x):
    far = lax.all_gather(x[None], "expert_0", tiled=True)
    near = jnp.broadcast_to(far[None], (NEAR_SIZE, *far.shape))
    return lax.all_to_all(near, NEAR, 0, 0)


def body(tokens, routes, gate_values, gate_weight, up_weight, down_weight):
    expert = lax.axis_index("expert_0")
    packed = call(pack_kernel, (32, 128), "pack", tokens.T)
    parts = spread(packed)

    matched = routes[:, :, None] == lax.broadcasted_iota(jnp.int32, (1, 1, EXPERTS), 2)
    combine_table = jnp.sum(jnp.where(matched, gate_values[:, :, None].astype(F32), 0.0), axis=1)
    weights = lax.dynamic_slice_in_dim(combine_table, expert, 1, 1)
    present = jnp.any(matched, axis=1)
    slot = jnp.cumsum(present.astype(jnp.int32), axis=0) - 1
    place = jnp.logical_and(
        present.T[:, None, :],
        slot.T[:, None, :] == lax.broadcasted_iota(jnp.int32, (1, SLOTS, 1), 1),
    ).astype(BF16)
    own = lax.dynamic_slice_in_dim(place, expert, 1, 0)[0]

    shape = (EXPERTS, NEAR_SIZE, 56, 128)
    pieces = call(
        gates_kernel, (SLOTS, 128), "gates",
        parts, gate_weight.reshape(shape), up_weight.reshape(shape), weights, own,
    )
    gathered = spread(pieces)
    return call(down_kernel, (56, 64), "down", gathered, down_weight.T, place).T


def solution(mesh):
    split = Mesh(mesh.devices.reshape(mesh.shape["dp"], EXPERTS, 2, 4), ("dp", *GROUP))
    return jax.shard_map(
        body,
        mesh=split,
        in_specs=(
            P("dp", GROUP),
            P("dp", None),
            P("dp", None),
            P(None, GROUP),
            P(None, GROUP),
            P(None, GROUP),
        ),
        out_specs=P("dp", GROUP),
        check_vma=False,
    )
```

```python
import jax
import jax.numpy as jnp
from jax import lax
from jax.experimental import pallas as pl
from jax.experimental.pallas import tpu as pltpu
from jax.sharding import Mesh
from jax.sharding import PartitionSpec as P

HIDDEN_SIZE = 1024
EXPERTS = 16
TOPK = 8
TOKENS = 64
SLOTS = 40
FEATURES = 56
NEAR_SIZE = 8
TALL = EXPERTS * FEATURES
ROWS = 304
GROUP = ("expert_0", "expert_1", "expert_2")
NEAR = ("expert_1", "expert_2")
LIMIT = pltpu.CompilerParams(vmem_limit_bytes=8 * 2**20)
VMEM = pl.BlockSpec(memory_space=pltpu.VMEM)
SMEM = pl.BlockSpec(memory_space=pltpu.SMEM)
COST = pl.CostEstimate(flops=10**10, bytes_accessed=6 * 10**7, transcendentals=0)
F32 = jnp.float32
BF16 = jnp.bfloat16


def dot(x, y, x_dim, y_dim):
    return lax.dot_general(x, y, (((x_dim,), (y_dim,)), ((), ())), preferred_element_type=F32)


def span(group):
    return group * ROWS, min((group + 1) * ROWS, TALL)


def pack_kernel(columns, packed):
    packed[:, :64] = columns[:32]
    packed[:24, 64:] = columns[32:]
    packed[24:, 64:] = jnp.zeros((8, 64), BF16)


def route(expert, routes, values, place, weights):
    earlier = lax.broadcasted_iota(jnp.int32, (TOKENS, TOKENS), 0)
    earlier = earlier < lax.broadcasted_iota(jnp.int32, (TOKENS, TOKENS), 1)
    earlier = jnp.where(earlier, 1.0, 0.0).astype(BF16)
    ids = lax.broadcasted_iota(jnp.int32, (EXPERTS, TOKENS), 0)
    slots = lax.broadcasted_iota(jnp.int32, (SLOTS, TOKENS), 0).astype(F32)
    table = jnp.zeros((EXPERTS, TOKENS), F32)
    present = jnp.zeros((EXPERTS, TOKENS), F32)
    for k in range(TOPK):
        matched = routes[k : k + 1, :] == ids
        table = jnp.where(matched, values[k : k + 1, :].astype(F32), table)
        present = jnp.where(matched, 1.0, present)
    slot = dot(present.astype(BF16), earlier, 1, 0)
    slot = jnp.where(present > 0.0, slot, -1.0)
    for e in range(EXPERTS):
        chosen = jnp.where(slot[e : e + 1, :] == slots, 1.0, 0.0)
        place[e * SLOTS : (e + 1) * SLOTS, :] = chosen.astype(BF16)
    mine = ids == expert
    own_slot = jnp.sum(jnp.where(mine, slot, 0.0), axis=0, keepdims=True)
    own_gate = jnp.sum(jnp.where(mine, table, 0.0), axis=0, keepdims=True)
    chosen = jnp.where(own_slot == slots, 1.0, 0.0)
    weights[...] = jnp.sum(chosen * own_gate, axis=1, keepdims=True)
    return chosen.astype(BF16)


def pick_kernel(expert, routes, values, far, out, place, weights):
    own = route(expert[0], routes, values, place, weights)
    blank = jnp.zeros((SLOTS, 64), BF16)
    halves = jnp.concatenate([own, blank], axis=1), jnp.concatenate([blank, own], axis=1)
    total = jnp.zeros((ROWS, 128), F32)
    for group in range(3):
        first, last = span(group)
        low, high = first // FEATURES, -(-last // FEATURES)
        above, below = group * SLOTS, 128 - (group + 1) * SLOTS
        sides = []
        for half in halves:
            chooser = [half, jnp.zeros((below, 128), BF16)]
            if above:
                chooser = [jnp.zeros((above, 128), BF16), *chooser]
            chooser = jnp.concatenate(chooser, axis=0)
            sides.append(dot(far[low * 32 : high * 32, :], chooser, 1, 1))
        rows = []
        for piece in range(low, high):
            for side, (start, stop) in enumerate(((0, 32), (32, FEATURES))):
                begin = max(first - piece * FEATURES, start)
                end = min(last - piece * FEATURES, stop)
                if begin < end:
                    base = (piece - low) * 32 - start
                    rows.append(sides[side][base + begin : base + end])
        if last - first < ROWS:
            rows.append(jnp.zeros((ROWS - (last - first), 128), F32))
        total = total + jnp.concatenate(rows, axis=0)
    result = total.astype(BF16)
    for near in range(NEAR_SIZE):
        out[near] = result


def gates_kernel(parts, gate, up, weights, pieces):
    totals = [jnp.zeros((128, 256), F32)] * 3
    for near in range(NEAR_SIZE):
        x = parts[near]
        w = [ref[:, near, :, :].reshape(TALL, 128) for ref in (gate, up)]
        w = jnp.concatenate(w, axis=1)
        for group in range(3):
            first, last = span(group)
            totals[group] = totals[group] + dot(x[: last - first], w[first:last], 0, 0)
    both = [totals[group][group * SLOTS : (group + 1) * SLOTS] for group in range(3)]
    both = both[0] + both[1] + both[2]
    gate_proj, up_proj = both[:, :128], both[:, 128:]
    silu = gate_proj / (1.0 + jnp.exp(-gate_proj))
    pieces[...] = (silu * up_proj * weights[...]).astype(BF16)


def down_kernel(gathered, down, place, out):
    rows = []
    for expert in range(EXPERTS):
        total = jnp.zeros((SLOTS, FEATURES), F32)
        for near in range(0, NEAR_SIZE, 2):
            pair = [gathered[near, expert], gathered[near + 1, expert]]
            low = expert * HIDDEN_SIZE + near * 128
            total = total + dot(jnp.concatenate(pair, axis=1), down[:, low : low + 256], 1, 1)
        rows.append(total)
    rows = jnp.concatenate(rows, axis=0)
    coarse = rows.astype(BF16)
    fine = (rows - coarse.astype(F32)).astype(BF16)
    out[...] = (dot(coarse, place[...], 0, 0) + dot(fine, place[...], 0, 0)).astype(BF16)


def call(kernel, name, shapes, args, **options):
    out = [jax.ShapeDtypeStruct(shape, dtype) for shape, dtype in shapes]
    return pl.pallas_call(kernel, out_shape=out, compiler_params=LIMIT, cost_estimate=COST, name=name, **options)(*args)


def body(tokens, routes, gate_values, gate_weight, up_weight, down_weight):
    expert = lax.axis_index("expert_0").reshape(1)
    (packed,) = call(pack_kernel, "pack", [((32, 128), BF16)], (tokens.T,))
    far = lax.all_gather(packed, "expert_0", tiled=True)
    near, place, weights = call(
        pick_kernel,
        "pick",
        [((NEAR_SIZE, ROWS, 128), BF16), ((EXPERTS * SLOTS, TOKENS), BF16), ((SLOTS, 1), F32)],
        (expert, routes.T, gate_values.T, far),
        in_specs=[SMEM, VMEM, VMEM, VMEM],
    )
    parts = lax.all_to_all(near, NEAR, 0, 0)
    shape = (EXPERTS, NEAR_SIZE, FEATURES, 128)
    (pieces,) = call(
        gates_kernel,
        "gates",
        [((SLOTS, 128), BF16)],
        (parts, gate_weight.reshape(shape), up_weight.reshape(shape), weights),
    )
    far = lax.all_gather(pieces[None], "expert_0", tiled=True)
    near = jnp.broadcast_to(far[None], (NEAR_SIZE, *far.shape))
    gathered = lax.all_to_all(near, NEAR, 0, 0)
    (out,) = call(
        down_kernel, "down", [((FEATURES, TOKENS), BF16)], (gathered, down_weight.T, place)
    )
    return out.T


def solution(mesh):
    split = Mesh(mesh.devices.reshape(mesh.shape["dp"], EXPERTS, 2, 4), ("dp", *GROUP))
    return jax.shard_map(
        body,
        mesh=split,
        in_specs=(
            P("dp", GROUP),
            P("dp", None),
            P("dp", None),
            P(None, GROUP),
            P(None, GROUP),
            P(None, GROUP),
        ),
        out_specs=P("dp", GROUP),
        check_vma=False,
    )
```

```python
import jax
import jax.numpy as jnp
from jax import lax
from jax.experimental import pallas as pl
from jax.experimental.pallas import tpu as pltpu
from jax.sharding import Mesh
from jax.sharding import PartitionSpec as P

HIDDEN_SIZE = 1024
EXPERTS = 16
TOPK = 8
TOKENS = 64
SLOTS = 40
FEATURES = 56
NEAR_SIZE = 8
TALL = EXPERTS * FEATURES
SPLIT = 32
GROUP = ("expert_0", "expert_1", "expert_2")
NEAR = ("expert_1", "expert_2")
LIMIT = pltpu.CompilerParams(vmem_limit_bytes=8 * 2**20)
VMEM = pl.BlockSpec(memory_space=pltpu.VMEM)
SMEM = pl.BlockSpec(memory_space=pltpu.SMEM)
COST = pl.CostEstimate(flops=10**10, bytes_accessed=6 * 10**7, transcendentals=0)
F32 = jnp.float32
BF16 = jnp.bfloat16


def dot(x, y, x_dim, y_dim):
    return lax.dot_general(x, y, (((x_dim,), (y_dim,)), ((), ())), preferred_element_type=F32)


def pack_kernel(columns, packed):
    packed[:, :64] = columns[:SPLIT]
    packed[: FEATURES - SPLIT, 64:] = columns[SPLIT:]
    packed[FEATURES - SPLIT :, 64:] = jnp.zeros((2 * SPLIT - FEATURES, 64), BF16)


def route(expert, routes, values, place, weights):
    earlier = lax.broadcasted_iota(jnp.int32, (TOKENS, TOKENS), 0)
    earlier = earlier < lax.broadcasted_iota(jnp.int32, (TOKENS, TOKENS), 1)
    earlier = jnp.where(earlier, 1.0, 0.0).astype(BF16)
    ids = lax.broadcasted_iota(jnp.int32, (EXPERTS, TOKENS), 0)
    slots = lax.broadcasted_iota(jnp.int32, (SLOTS, TOKENS), 0).astype(F32)
    table = jnp.zeros((EXPERTS, TOKENS), F32)
    present = jnp.zeros((EXPERTS, TOKENS), F32)
    for k in range(TOPK):
        matched = routes[k : k + 1, :] == ids
        table = jnp.where(matched, values[k : k + 1, :].astype(F32), table)
        present = jnp.where(matched, 1.0, present)
    slot = dot(present.astype(BF16), earlier, 1, 0)
    slot = jnp.where(present > 0.0, slot, -1.0)
    for e in range(EXPERTS):
        chosen = jnp.where(slot[e : e + 1, :] == slots, 1.0, 0.0)
        place[e * SLOTS : (e + 1) * SLOTS, :] = chosen.astype(BF16)
    mine = ids == expert
    own_slot = jnp.sum(jnp.where(mine, slot, 0.0), axis=0, keepdims=True)
    own_gate = jnp.sum(jnp.where(mine, table, 0.0), axis=0, keepdims=True)
    chosen = jnp.where(own_slot == slots, 1.0, 0.0)
    weights[...] = jnp.sum(chosen * own_gate, axis=1, keepdims=True)
    return chosen.astype(BF16)


def pick_kernel(expert, routes, values, far, out, place, weights):
    own = route(expert[0], routes, values, place, weights)
    blank = jnp.zeros((SLOTS, 64), BF16)
    low = dot(jnp.concatenate([own, blank], axis=1), far[...].reshape(EXPERTS * SPLIT, 128), 1, 1)
    high = far[:, : FEATURES - SPLIT, :].reshape(EXPERTS * (FEATURES - SPLIT), 128)
    high = dot(jnp.concatenate([blank, own], axis=1), high, 1, 1)
    picked = jnp.concatenate([low, high], axis=1).astype(BF16)
    for near in range(NEAR_SIZE):
        out[near] = picked


def gates_kernel(parts, gate, up, weights, pieces):
    total = jnp.zeros((SLOTS, 256), F32)
    for near in range(NEAR_SIZE):
        w = [ref[:, near, :SPLIT, :].reshape(EXPERTS * SPLIT, 128) for ref in (gate, up)]
        total = total + dot(parts[near, :, : EXPERTS * SPLIT], jnp.concatenate(w, axis=1), 1, 0)
        w = [ref[:, near, SPLIT:, :].reshape(TALL - EXPERTS * SPLIT, 128) for ref in (gate, up)]
        total = total + dot(parts[near, :, EXPERTS * SPLIT :], jnp.concatenate(w, axis=1), 1, 0)
    gate_proj, up_proj = total[:, :128], total[:, 128:]
    silu = gate_proj / (1.0 + jnp.exp(-gate_proj))
    pieces[...] = (silu * up_proj * weights[...]).astype(BF16)


def down_kernel(gathered, down, place, out):
    rows = []
    for expert in range(EXPERTS):
        total = jnp.zeros((SLOTS, FEATURES), F32)
        for near in range(0, NEAR_SIZE, 2):
            pair = [gathered[near, expert], gathered[near + 1, expert]]
            low = expert * HIDDEN_SIZE + near * 128
            total = total + dot(jnp.concatenate(pair, axis=1), down[:, low : low + 256], 1, 1)
        rows.append(total)
    rows = jnp.concatenate(rows, axis=0)
    coarse = rows.astype(BF16)
    fine = (rows - coarse.astype(F32)).astype(BF16)
    out[...] = (dot(coarse, place[...], 0, 0) + dot(fine, place[...], 0, 0)).astype(BF16)


def call(kernel, name, shapes, args, **options):
    out = [jax.ShapeDtypeStruct(shape, dtype) for shape, dtype in shapes]
    return pl.pallas_call(
        kernel, out_shape=out, compiler_params=LIMIT, cost_estimate=COST, name=name, **options
    )(*args)


def body(tokens, routes, gate_values, gate_weight, up_weight, down_weight):
    expert = lax.axis_index("expert_0").reshape(1)
    (packed,) = call(pack_kernel, "pack", [((SPLIT, 128), BF16)], (tokens.T,))
    far = lax.all_gather(packed[None], "expert_0", tiled=True)
    near, place, weights = call(
        pick_kernel,
        "pick",
        [((NEAR_SIZE, SLOTS, TALL), BF16), ((EXPERTS * SLOTS, TOKENS), BF16), ((SLOTS, 1), F32)],
        (expert, routes.T, gate_values.T, far),
        in_specs=[SMEM, VMEM, VMEM, VMEM],
    )
    parts = lax.all_to_all(near, NEAR, 0, 0)
    shape = (EXPERTS, NEAR_SIZE, FEATURES, 128)
    (pieces,) = call(
        gates_kernel,
        "gates",
        [((SLOTS, 128), BF16)],
        (parts, gate_weight.reshape(shape), up_weight.reshape(shape), weights),
    )
    far = lax.all_gather(pieces[None], "expert_0", tiled=True)
    near = jnp.broadcast_to(far[None], (NEAR_SIZE, *far.shape))
    gathered = lax.all_to_all(near, NEAR, 0, 0)
    (out,) = call(
        down_kernel, "down", [((FEATURES, TOKENS), BF16)], (gathered, down_weight.T, place)
    )
    return out.T


def solution(mesh):
    split = Mesh(mesh.devices.reshape(mesh.shape["dp"], EXPERTS, 2, 4), ("dp", *GROUP))
    return jax.shard_map(
        body,
        mesh=split,
        in_specs=(
            P("dp", GROUP),
            P("dp", None),
            P("dp", None),
            P(None, GROUP),
            P(None, GROUP),
            P(None, GROUP),
        ),
        out_specs=P("dp", GROUP),
        check_vma=False,
    )
```

```python
import jax
import jax.numpy as jnp
from jax import lax
from jax.experimental import pallas as pl
from jax.experimental.pallas import tpu as pltpu
from jax.sharding import Mesh
from jax.sharding import PartitionSpec as P

HIDDEN_SIZE = 1024
EXPERTS = 16
TOPK = 8
TOKENS = 64
SLOTS = 40
FEATURES = 56
NEAR_SIZE = 8
TALL = EXPERTS * FEATURES
SPLIT = 32
FILLED = TOKENS * TOPK
WINDOW = 48
GROUP = ("expert_0", "expert_1", "expert_2")
NEAR = ("expert_1", "expert_2")
LIMIT = pltpu.CompilerParams(vmem_limit_bytes=8 * 2**20)
VMEM = pl.BlockSpec(memory_space=pltpu.VMEM)
SMEM = pl.BlockSpec(memory_space=pltpu.SMEM)
COST = pl.CostEstimate(flops=10**10, bytes_accessed=6 * 10**7, transcendentals=0)
F32 = jnp.float32
BF16 = jnp.bfloat16


def dot(x, y, x_dim, y_dim):
    return lax.dot_general(x, y, (((x_dim,), (y_dim,)), ((), ())), preferred_element_type=F32)


def pack_kernel(columns, packed):
    packed[:, :64] = columns[:SPLIT]
    packed[: FEATURES - SPLIT, 64:] = columns[SPLIT:]
    packed[FEATURES - SPLIT :, 64:] = jnp.zeros((2 * SPLIT - FEATURES, 64), BF16)


def route(expert, routes, values, place, weights, starts):
    earlier = lax.broadcasted_iota(jnp.int32, (TOKENS, TOKENS), 0)
    earlier = earlier < lax.broadcasted_iota(jnp.int32, (TOKENS, TOKENS), 1)
    earlier = jnp.where(earlier, 1.0, 0.0).astype(BF16)
    ids = lax.broadcasted_iota(jnp.int32, (EXPERTS, TOKENS), 0)
    slots = lax.broadcasted_iota(jnp.int32, (SLOTS, TOKENS), 0).astype(F32)
    table = jnp.zeros((EXPERTS, TOKENS), F32)
    present = jnp.zeros((EXPERTS, TOKENS), F32)
    for k in range(TOPK):
        matched = routes[k : k + 1, :] == ids
        table = jnp.where(matched, values[k : k + 1, :].astype(F32), table)
        present = jnp.where(matched, 1.0, present)
    slot = dot(present.astype(BF16), earlier, 1, 0)
    slot = jnp.where(present > 0.0, slot, -1.0)
    before = lax.broadcasted_iota(jnp.int32, (EXPERTS, EXPERTS), 0)
    before = before > lax.broadcasted_iota(jnp.int32, (EXPERTS, EXPERTS), 1)
    start = dot(jnp.where(before, 1.0, 0.0).astype(BF16), present.astype(BF16), 1, 0)
    start = jnp.sum(start, axis=1, keepdims=True)
    window = jnp.minimum(jnp.floor(start * 0.125) * 8.0, float(FILLED - WINDOW))
    shifted = jnp.where(present > 0.0, slot + (start - window), -1.0)
    rows = lax.broadcasted_iota(jnp.int32, (WINDOW, TOKENS), 0).astype(F32)
    for e in range(EXPERTS):
        chosen = jnp.where(shifted[e : e + 1, :] == rows, 1.0, 0.0)
        place[e * WINDOW : (e + 1) * WINDOW, :] = chosen.astype(BF16)
        starts[e] = jnp.sum(start[e : e + 1, :]).astype(jnp.int32)
    mine = ids == expert
    own_slot = jnp.sum(jnp.where(mine, slot, 0.0), axis=0, keepdims=True)
    own_gate = jnp.sum(jnp.where(mine, table, 0.0), axis=0, keepdims=True)
    chosen = jnp.where(own_slot == slots, 1.0, 0.0)
    weights[...] = jnp.sum(chosen * own_gate, axis=1, keepdims=True)
    return chosen.astype(BF16)


def pick_kernel(expert, routes, values, far, out, place, weights, starts):
    own = route(expert[0], routes, values, place, weights, starts)
    blank = jnp.zeros((SLOTS, 64), BF16)
    low = dot(jnp.concatenate([own, blank], axis=1), far[...].reshape(EXPERTS * SPLIT, 128), 1, 1)
    high = far[:, : FEATURES - SPLIT, :].reshape(EXPERTS * (FEATURES - SPLIT), 128)
    high = dot(jnp.concatenate([blank, own], axis=1), high, 1, 1)
    picked = jnp.concatenate([low, high], axis=1).astype(BF16)
    for near in range(NEAR_SIZE):
        out[near] = picked


def gates_kernel(parts, gate, up, weights, pieces):
    total = jnp.zeros((SLOTS, 256), F32)
    for near in range(NEAR_SIZE):
        w = [ref[:, near, :SPLIT, :].reshape(EXPERTS * SPLIT, 128) for ref in (gate, up)]
        total = total + dot(parts[near, :, : EXPERTS * SPLIT], jnp.concatenate(w, axis=1), 1, 0)
        w = [ref[:, near, SPLIT:, :].reshape(TALL - EXPERTS * SPLIT, 128) for ref in (gate, up)]
        total = total + dot(parts[near, :, EXPERTS * SPLIT :], jnp.concatenate(w, axis=1), 1, 0)
    gate_proj, up_proj = total[:, :128], total[:, 128:]
    silu = gate_proj / (1.0 + jnp.exp(-gate_proj))
    pieces[...] = (silu * up_proj * weights[...]).astype(BF16)


def close_kernel(starts, far, out, rows):
    for e in range(EXPERTS):
        piece = far[e * SLOTS : (e + 1) * SLOTS, :].astype(F32)
        rows[pl.ds(starts[e], SLOTS), :] = piece
    closed = rows[:FILLED, :].astype(BF16)
    for near in range(NEAR_SIZE):
        out[near] = closed


def down_kernel(starts, gathered, down, place, out):
    rows = []
    for e in range(EXPERTS):
        first = pl.multiple_of(jnp.minimum(starts[e] // 8 * 8, FILLED - WINDOW), 8)
        total = jnp.zeros((WINDOW, FEATURES), F32)
        for near in range(0, NEAR_SIZE, 2):
            pair = [gathered[near + i, pl.ds(first, WINDOW), :] for i in range(2)]
            low = e * HIDDEN_SIZE + near * 128
            total = total + dot(jnp.concatenate(pair, axis=1), down[:, low : low + 256], 1, 1)
        rows.append(total)
    rows = jnp.concatenate(rows, axis=0)
    coarse = rows.astype(BF16)
    fine = (rows - coarse.astype(F32)).astype(BF16)
    out[...] = (dot(coarse, place[...], 0, 0) + dot(fine, place[...], 0, 0)).astype(BF16)


def call(kernel, name, shapes, args, **options):
    out = [jax.ShapeDtypeStruct(shape, dtype) for shape, dtype in shapes]
    return pl.pallas_call(
        kernel, out_shape=out, compiler_params=LIMIT, cost_estimate=COST, name=name, **options
    )(*args)


def body(tokens, routes, gate_values, gate_weight, up_weight, down_weight):
    expert = lax.axis_index("expert_0").reshape(1)
    (packed,) = call(pack_kernel, "pack", [((SPLIT, 128), BF16)], (tokens.T,))
    far = lax.all_gather(packed[None], "expert_0", tiled=True)
    near, place, weights, starts = call(
        pick_kernel,
        "pick",
        [((NEAR_SIZE, SLOTS, TALL), BF16), ((EXPERTS * WINDOW, TOKENS), BF16), ((SLOTS, 1), F32), ((EXPERTS,), jnp.int32)],
        (expert, routes.T, gate_values.T, far),
        in_specs=[SMEM, VMEM, VMEM, VMEM],
        out_specs=[VMEM, VMEM, VMEM, SMEM],
    )
    parts = lax.all_to_all(near, NEAR, 0, 0)
    shape = (EXPERTS, NEAR_SIZE, FEATURES, 128)
    (pieces,) = call(
        gates_kernel,
        "gates",
        [((SLOTS, 128), BF16)],
        (parts, gate_weight.reshape(shape), up_weight.reshape(shape), weights),
    )
    far = lax.all_gather(pieces, "expert_0", tiled=True)
    (near,) = call(
        close_kernel,
        "close",
        [((NEAR_SIZE, FILLED, 128), BF16)],
        (starts, far),
        in_specs=[SMEM, VMEM],
        scratch_shapes=[pltpu.VMEM((FILLED + SLOTS, 128), F32)],
    )
    gathered = lax.all_to_all(near, NEAR, 0, 0)
    (out,) = call(
        down_kernel,
        "down",
        [((FEATURES, TOKENS), BF16)],
        (starts, gathered, down_weight.T, place),
        in_specs=[SMEM, VMEM, VMEM, VMEM],
    )
    return out.T


def solution(mesh):
    split = Mesh(mesh.devices.reshape(mesh.shape["dp"], EXPERTS, 2, 4), ("dp", *GROUP))
    return jax.shard_map(
        body,
        mesh=split,
        in_specs=(
            P("dp", GROUP),
            P("dp", None),
            P("dp", None),
            P(None, GROUP),
            P(None, GROUP),
            P(None, GROUP),
        ),
        out_specs=P("dp", GROUP),
        check_vma=False,
    )
```

```python
import jax
import jax.numpy as jnp
from jax import lax
from jax.experimental import pallas as pl
from jax.experimental.pallas import tpu as pltpu
from jax.sharding import Mesh
from jax.sharding import PartitionSpec as P

HIDDEN_SIZE = 1024
EXPERTS = 16
TOPK = 8
TOKENS = 64
SLOTS = 40
FEATURES = 56
NEAR_SIZE = 8
TALL = EXPERTS * FEATURES
SPLIT = 32
FILLED = TOKENS * TOPK
WINDOW = 48
GROUP = ("expert_0", "expert_1", "expert_2")
NEAR = ("expert_1", "expert_2")
LIMIT = pltpu.CompilerParams(vmem_limit_bytes=8 * 2**20)
VMEM = pl.BlockSpec(memory_space=pltpu.VMEM)
SMEM = pl.BlockSpec(memory_space=pltpu.SMEM)
COST = pl.CostEstimate(flops=10**10, bytes_accessed=6 * 10**7, transcendentals=0)
F32 = jnp.float32
BF16 = jnp.bfloat16


def dot(x, y, x_dim, y_dim):
    return lax.dot_general(x, y, (((x_dim,), (y_dim,)), ((), ())), preferred_element_type=F32)


def pack_kernel(columns, packed):
    packed[:, :64] = columns[:SPLIT]
    packed[: FEATURES - SPLIT, 64:] = columns[SPLIT:]
    packed[FEATURES - SPLIT :, 64:] = jnp.zeros((2 * SPLIT - FEATURES, 64), BF16)


def route(expert, routes, values, place, weights, starts):
    earlier = lax.broadcasted_iota(jnp.int32, (TOKENS, TOKENS), 0)
    earlier = earlier < lax.broadcasted_iota(jnp.int32, (TOKENS, TOKENS), 1)
    earlier = jnp.where(earlier, 1.0, 0.0).astype(BF16)
    ids = lax.broadcasted_iota(jnp.int32, (EXPERTS, TOKENS), 0)
    slots = lax.broadcasted_iota(jnp.int32, (SLOTS, TOKENS), 0).astype(F32)
    table = jnp.zeros((EXPERTS, TOKENS), F32)
    present = jnp.zeros((EXPERTS, TOKENS), F32)
    for k in range(TOPK):
        matched = routes[k : k + 1, :] == ids
        table = jnp.where(matched, values[k : k + 1, :].astype(F32), table)
        present = jnp.where(matched, 1.0, present)
    slot = dot(present.astype(BF16), earlier, 1, 0)
    slot = jnp.where(present > 0.0, slot, -1.0)
    before = lax.broadcasted_iota(jnp.int32, (EXPERTS, EXPERTS), 0)
    before = before > lax.broadcasted_iota(jnp.int32, (EXPERTS, EXPERTS), 1)
    start = dot(jnp.where(before, 1.0, 0.0).astype(BF16), present.astype(BF16), 1, 0)
    start = jnp.sum(start, axis=1, keepdims=True)
    window = jnp.minimum(jnp.floor(start * 0.125) * 8.0, float(FILLED - WINDOW))
    shifted = jnp.where(present > 0.0, slot + (start - window), -1.0)
    rows = lax.broadcasted_iota(jnp.int32, (WINDOW, TOKENS), 0).astype(F32)
    for e in range(EXPERTS):
        chosen = jnp.where(shifted[e : e + 1, :] == rows, 1.0, 0.0)
        place[e * WINDOW : (e + 1) * WINDOW, :] = chosen.astype(BF16)
    counts = dot(jnp.ones((8, TOKENS), BF16), present.astype(BF16), 1, 1).astype(BF16)
    starts[...] = dot(counts, jnp.where(before, 1.0, 0.0).astype(BF16), 1, 1)[:1].astype(jnp.int32)
    mine = ids == expert
    own_slot = jnp.sum(jnp.where(mine, slot, 0.0), axis=0, keepdims=True)
    own_gate = jnp.sum(jnp.where(mine, table, 0.0), axis=0, keepdims=True)
    chosen = jnp.where(own_slot == slots, 1.0, 0.0)
    weights[...] = jnp.sum(chosen * own_gate, axis=1, keepdims=True)
    return chosen.astype(BF16)


def pick_kernel(expert, routes, values, far, out, place, weights, starts):
    own = route(expert[0], routes, values, place, weights, starts)
    blank = jnp.zeros((SLOTS, 64), BF16)
    low = dot(jnp.concatenate([own, blank], axis=1), far[...].reshape(EXPERTS * SPLIT, 128), 1, 1)
    high = far[:, : FEATURES - SPLIT, :].reshape(EXPERTS * (FEATURES - SPLIT), 128)
    high = dot(jnp.concatenate([blank, own], axis=1), high, 1, 1)
    picked = jnp.concatenate([low, high], axis=1).astype(BF16)
    for near in range(NEAR_SIZE):
        out[near] = picked


def gates_kernel(parts, gate, up, weights, pieces):
    total = jnp.zeros((SLOTS, 256), F32)
    for near in range(NEAR_SIZE):
        w = [ref[:, near, :SPLIT, :].reshape(EXPERTS * SPLIT, 128) for ref in (gate, up)]
        total = total + dot(parts[near, :, : EXPERTS * SPLIT], jnp.concatenate(w, axis=1), 1, 0)
        w = [ref[:, near, SPLIT:, :].reshape(TALL - EXPERTS * SPLIT, 128) for ref in (gate, up)]
        total = total + dot(parts[near, :, EXPERTS * SPLIT :], jnp.concatenate(w, axis=1), 1, 0)
    gate_proj, up_proj = total[:, :128], total[:, 128:]
    silu = gate_proj / (1.0 + jnp.exp(-gate_proj))
    pieces[...] = (silu * up_proj * weights[...]).astype(BF16)


def close_kernel(starts, far, out, rows):
    for e in range(EXPERTS):
        piece = far[e * SLOTS : (e + 1) * SLOTS, :].astype(F32)
        rows[pl.ds(starts[0, e], SLOTS), :] = piece
    closed = rows[:FILLED, :].astype(BF16)
    for near in range(NEAR_SIZE):
        out[near] = closed


def down_kernel(starts, gathered, down, place, out):
    rows = []
    for e in range(EXPERTS):
        first = pl.multiple_of(jnp.minimum(starts[0, e] // 8 * 8, FILLED - WINDOW), 8)
        total = jnp.zeros((WINDOW, FEATURES), F32)
        for near in range(0, NEAR_SIZE, 2):
            pair = [gathered[near + i, pl.ds(first, WINDOW), :] for i in range(2)]
            low = e * HIDDEN_SIZE + near * 128
            total = total + dot(jnp.concatenate(pair, axis=1), down[:, low : low + 256], 1, 1)
        rows.append(total)
    rows = jnp.concatenate(rows, axis=0)
    coarse = rows.astype(BF16)
    fine = (rows - coarse.astype(F32)).astype(BF16)
    out[...] = (dot(coarse, place[...], 0, 0) + dot(fine, place[...], 0, 0)).astype(BF16)


def call(kernel, name, shapes, args, **options):
    out = [jax.ShapeDtypeStruct(shape, dtype) for shape, dtype in shapes]
    return pl.pallas_call(
        kernel, out_shape=out, compiler_params=LIMIT, cost_estimate=COST, name=name, **options
    )(*args)


def body(tokens, routes, gate_values, gate_weight, up_weight, down_weight):
    expert = lax.axis_index("expert_0").reshape(1)
    (packed,) = call(pack_kernel, "pack", [((SPLIT, 128), BF16)], (tokens.T,))
    far = lax.all_gather(packed[None], "expert_0", tiled=True)
    near, place, weights, starts = call(
        pick_kernel,
        "pick",
        [((NEAR_SIZE, SLOTS, TALL), BF16), ((EXPERTS * WINDOW, TOKENS), BF16), ((SLOTS, 1), F32), ((1, EXPERTS), jnp.int32)],
        (expert, routes.T, gate_values.T, far),
        in_specs=[SMEM, VMEM, VMEM, VMEM],
    )
    parts = lax.all_to_all(near, NEAR, 0, 0)
    shape = (EXPERTS, NEAR_SIZE, FEATURES, 128)
    (pieces,) = call(
        gates_kernel,
        "gates",
        [((SLOTS, 128), BF16)],
        (parts, gate_weight.reshape(shape), up_weight.reshape(shape), weights),
    )
    far = lax.all_gather(pieces, "expert_0", tiled=True)
    (near,) = call(
        close_kernel,
        "close",
        [((NEAR_SIZE, FILLED, 128), BF16)],
        (starts, far),
        in_specs=[SMEM, VMEM],
        scratch_shapes=[pltpu.VMEM((FILLED + SLOTS, 128), F32)],
    )
    gathered = lax.all_to_all(near, NEAR, 0, 0)
    (out,) = call(
        down_kernel,
        "down",
        [((FEATURES, TOKENS), BF16)],
        (starts, gathered, down_weight.T, place),
        in_specs=[SMEM, VMEM, VMEM, VMEM],
    )
    return out.T


def solution(mesh):
    split = Mesh(mesh.devices.reshape(mesh.shape["dp"], EXPERTS, 2, 4), ("dp", *GROUP))
    return jax.shard_map(
        body,
        mesh=split,
        in_specs=(
            P("dp", GROUP),
            P("dp", None),
            P("dp", None),
            P(None, GROUP),
            P(None, GROUP),
            P(None, GROUP),
        ),
        out_specs=P("dp", GROUP),
        check_vma=False,
    )
```

```python
import jax
import jax.numpy as jnp
from jax import lax
from jax.experimental import pallas as pl
from jax.experimental.pallas import tpu as pltpu
from jax.sharding import Mesh
from jax.sharding import PartitionSpec as P

HIDDEN_SIZE = 1024
EXPERTS = 16
TOPK = 8
TOKENS = 64
SLOTS = 40
FEATURES = 56
NEAR_SIZE = 8
TALL = EXPERTS * FEATURES
SPLIT = 32
FILLED = TOKENS * TOPK
WINDOW = 48
GROUP = ("expert_0", "expert_1", "expert_2")
NEAR = ("expert_1", "expert_2")
LIMIT = pltpu.CompilerParams(vmem_limit_bytes=8 * 2**20)
VMEM = pl.BlockSpec(memory_space=pltpu.VMEM)
SMEM = pl.BlockSpec(memory_space=pltpu.SMEM)
COST = pl.CostEstimate(flops=10**10, bytes_accessed=6 * 10**7, transcendentals=0)
F32 = jnp.float32
BF16 = jnp.bfloat16


def dot(x, y, x_dim, y_dim):
    return lax.dot_general(x, y, (((x_dim,), (y_dim,)), ((), ())), preferred_element_type=F32)


def pack_kernel(columns, packed):
    packed[:, :64] = columns[:SPLIT]
    packed[: FEATURES - SPLIT, 64:] = columns[SPLIT:]
    packed[FEATURES - SPLIT :, 64:] = jnp.zeros((2 * SPLIT - FEATURES, 64), BF16)


def route(expert, routes, values, place, weights, starts):
    earlier = lax.broadcasted_iota(jnp.int32, (TOKENS, TOKENS), 0)
    earlier = earlier < lax.broadcasted_iota(jnp.int32, (TOKENS, TOKENS), 1)
    earlier = jnp.where(earlier, 1.0, 0.0).astype(BF16)
    ids = lax.broadcasted_iota(jnp.int32, (EXPERTS, TOKENS), 0)
    slots = lax.broadcasted_iota(jnp.int32, (SLOTS, TOKENS), 0).astype(F32)
    table = jnp.zeros((EXPERTS, TOKENS), F32)
    present = jnp.zeros((EXPERTS, TOKENS), F32)
    for k in range(TOPK):
        matched = routes[k : k + 1, :] == ids
        table = jnp.where(matched, values[k : k + 1, :].astype(F32), table)
        present = jnp.where(matched, 1.0, present)
    slot = dot(present.astype(BF16), earlier, 1, 0)
    slot = jnp.where(present > 0.0, slot, -1.0)
    before = lax.broadcasted_iota(jnp.int32, (EXPERTS, EXPERTS), 0)
    before = before > lax.broadcasted_iota(jnp.int32, (EXPERTS, EXPERTS), 1)
    start = dot(jnp.where(before, 1.0, 0.0).astype(BF16), present.astype(BF16), 1, 0)
    start = jnp.sum(start, axis=1, keepdims=True)
    window = jnp.minimum(jnp.floor(start * 0.125) * 8.0, float(FILLED - WINDOW))
    shifted = jnp.where(present > 0.0, slot + (start - window), -1.0)
    rows = lax.broadcasted_iota(jnp.int32, (WINDOW, TOKENS), 0).astype(F32)
    for e in range(EXPERTS):
        chosen = jnp.where(shifted[e : e + 1, :] == rows, 1.0, 0.0)
        place[e * WINDOW : (e + 1) * WINDOW, :] = chosen.astype(BF16)
    counts = dot(jnp.ones((8, TOKENS), BF16), present.astype(BF16), 1, 1).astype(BF16)
    row = dot(counts, jnp.where(before, 1.0, 0.0).astype(BF16), 1, 1)[:1]
    starts[:1] = row.astype(jnp.int32)
    starts[1:] = jnp.minimum(jnp.floor(row * 0.125) * 8.0, float(FILLED - WINDOW)).astype(jnp.int32)
    mine = ids == expert
    own_slot = jnp.sum(jnp.where(mine, slot, 0.0), axis=0, keepdims=True)
    own_gate = jnp.sum(jnp.where(mine, table, 0.0), axis=0, keepdims=True)
    chosen = jnp.where(own_slot == slots, 1.0, 0.0)
    weights[...] = jnp.sum(chosen * own_gate, axis=1, keepdims=True)
    return chosen.astype(BF16)


def pick_kernel(expert, routes, values, far, out, place, weights, starts):
    own = route(expert[0], routes, values, place, weights, starts)
    blank = jnp.zeros((SLOTS, 64), BF16)
    low = dot(jnp.concatenate([own, blank], axis=1), far[...].reshape(EXPERTS * SPLIT, 128), 1, 1)
    high = far[:, : FEATURES - SPLIT, :].reshape(EXPERTS * (FEATURES - SPLIT), 128)
    high = dot(jnp.concatenate([blank, own], axis=1), high, 1, 1)
    picked = jnp.concatenate([low, high], axis=1).astype(BF16)
    for near in range(NEAR_SIZE):
        out[near] = picked


def gates_kernel(parts, gate, up, weights, pieces):
    total = jnp.zeros((SLOTS, 256), F32)
    for near in range(NEAR_SIZE):
        w = [ref[:, near, :SPLIT, :].reshape(EXPERTS * SPLIT, 128) for ref in (gate, up)]
        total = total + dot(parts[near, :, : EXPERTS * SPLIT], jnp.concatenate(w, axis=1), 1, 0)
        w = [ref[:, near, SPLIT:, :].reshape(TALL - EXPERTS * SPLIT, 128) for ref in (gate, up)]
        total = total + dot(parts[near, :, EXPERTS * SPLIT :], jnp.concatenate(w, axis=1), 1, 0)
    gate_proj, up_proj = total[:, :128], total[:, 128:]
    silu = gate_proj / (1.0 + jnp.exp(-gate_proj))
    pieces[...] = (silu * up_proj * weights[...]).astype(BF16)


def close_kernel(starts, far, out, rows):
    for e in range(EXPERTS):
        piece = far[e * SLOTS : (e + 1) * SLOTS, :].astype(F32)
        rows[pl.ds(starts[0, e], SLOTS), :] = piece
    closed = rows[:FILLED, :].astype(BF16)
    for near in range(NEAR_SIZE):
        out[near] = closed


def down_kernel(starts, gathered, down, place, out):
    rows = []
    for e in range(EXPERTS):
        first = pl.multiple_of(starts[1, e], 8)
        near = [gathered[i, pl.ds(first, WINDOW), :] for i in range(NEAR_SIZE)]
        low = e * HIDDEN_SIZE
        rows.append(dot(jnp.concatenate(near, axis=1), down[:, low : low + HIDDEN_SIZE], 1, 1))
    rows = jnp.concatenate(rows, axis=0)
    coarse = rows.astype(BF16)
    fine = (rows - coarse.astype(F32)).astype(BF16)
    out[...] = (dot(coarse, place[...], 0, 0) + dot(fine, place[...], 0, 0)).astype(BF16)


def call(kernel, name, shapes, args, **options):
    out = [jax.ShapeDtypeStruct(shape, dtype) for shape, dtype in shapes]
    return pl.pallas_call(
        kernel, out_shape=out, compiler_params=LIMIT, cost_estimate=COST, name=name, **options
    )(*args)


def body(tokens, routes, gate_values, gate_weight, up_weight, down_weight):
    expert = lax.axis_index("expert_0").reshape(1)
    (packed,) = call(pack_kernel, "pack", [((SPLIT, 128), BF16)], (tokens.T,))
    far = lax.all_gather(packed[None], "expert_0", tiled=True)
    near, place, weights, starts = call(
        pick_kernel,
        "pick",
        [((NEAR_SIZE, SLOTS, TALL), BF16), ((EXPERTS * WINDOW, TOKENS), BF16), ((SLOTS, 1), F32), ((2, EXPERTS), jnp.int32)],
        (expert, routes.T, gate_values.T, far),
        in_specs=[SMEM, VMEM, VMEM, VMEM],
    )
    parts = lax.all_to_all(near, NEAR, 0, 0)
    shape = (EXPERTS, NEAR_SIZE, FEATURES, 128)
    (pieces,) = call(
        gates_kernel,
        "gates",
        [((SLOTS, 128), BF16)],
        (parts, gate_weight.reshape(shape), up_weight.reshape(shape), weights),
    )
    far = lax.all_gather(pieces, "expert_0", tiled=True)
    (near,) = call(
        close_kernel,
        "close",
        [((NEAR_SIZE, FILLED, 128), BF16)],
        (starts, far),
        in_specs=[SMEM, VMEM],
        scratch_shapes=[pltpu.VMEM((FILLED + SLOTS, 128), F32)],
    )
    gathered = lax.all_to_all(near, NEAR, 0, 0)
    (out,) = call(
        down_kernel,
        "down",
        [((FEATURES, TOKENS), BF16)],
        (starts, gathered, down_weight.T, place),
        in_specs=[SMEM, VMEM, VMEM, VMEM],
    )
    return out.T


def solution(mesh):
    split = Mesh(mesh.devices.reshape(mesh.shape["dp"], EXPERTS, 2, 4), ("dp", *GROUP))
    return jax.shard_map(
        body,
        mesh=split,
        in_specs=(
            P("dp", GROUP),
            P("dp", None),
            P("dp", None),
            P(None, GROUP),
            P(None, GROUP),
            P(None, GROUP),
        ),
        out_specs=P("dp", GROUP),
        check_vma=False,
    )
```
